256 devices in a mesh: section: 16 (over x, y), tensor: 16 (over z, core).
Axes of the slice: x: 4, y: 4, z: 8, core: 2. Of those that a mesh axis runs over, the one named last changes fastest.
Arguments:
- token_ids: int32 [3, 48], replicated, may hold values from 0 to 31999
- emb_table: bfloat16 [32000, 4096], P('section', 'tensor'), may hold values from -6 to 6
- attn_gain: bfloat16 [16, 4096], P('section'), may hold values from 0.25 to 1.75
- query_weight: bfloat16 [16, 4096, 4096], P('section', None, 'tensor'), may hold values from -8 to 8
- key_weight: bfloat16 [16, 4096, 4096], P('section', None, 'tensor'), may hold values from -8 to 8
- value_weight: bfloat16 [16, 4096, 4096], P('section', None, 'tensor'), may hold values from -0.09375 to 0.09375
- mix_weight: float32 [16, 32], P('section', 'tensor'), may hold values from 0.2 to 0.8
- out_weight: bfloat16 [16, 4096, 4096], P('section', 'tensor'), may hold values from -0.125 to 0.125
Outputs:
- layer_outputs: bfloat16 [16, 3, 48, 4096], P('section', None, None, 'tensor')
The draws below stay inside these ranges and needn't reach their ends.
All inputs are finite; a program needn't handle non-finite values.
Results may differ from the reference program's by a relative error of at most 0.033.
Values may be sent and summed in bfloat16 or wider, within the bound.
A program may use at most 64 MiB of HBM per device.

```python
import jax
import jax.numpy as jnp
from jax import lax

D = 4096
HEADS = 32
HEAD_DIM = 128
VOCAB = 32000
MICRO = 3
SEQ = 48
LAYERS = 16
N_TENSOR = 16


def weight_pair(key):
    query_key = jax.random.fold_in(key, 101)
    other_key = jax.random.fold_in(key, 202)
    shape = (LAYERS, D, HEADS * HEAD_DIM)
    base_draw = jax.random.normal(query_key, shape, jnp.float32) * D ** (-0.5)
    other_draw = jax.random.normal(other_key, shape, jnp.float32) * D ** (-0.5)
    return (base_draw, other_draw)


def draw_query_weight(key, part):
    return jnp.clip(weight_pair(key)[0], -8.0, 8.0).astype(jnp.bfloat16)


def draw_key_weight(key, part):
    return jnp.clip(weight_pair(key)[1], -8.0, 8.0).astype(jnp.bfloat16)


def plant(drawn, own_key, low, top_value):
    dims = drawn.shape
    spot = [jax.random.randint(jax.random.fold_in(own_key, axis), (), 0, dims[axis]) for axis in range(len(dims))]
    drawn = drawn.at[tuple(spot)].set(low)
    longest = dims.index(max(dims))
    spot[longest] = (spot[longest] + 1) % dims[longest]
    return drawn.at[tuple(spot)].set(top_value)


def strengthened(result, key, source, target, parts, factor):
    def block_of(axis_at):
        return (jnp.arange(result.shape[axis_at]) // (result.shape[axis_at] // parts)).reshape((-1,) + (1,) * (result.ndim - 1 - axis_at))

    near = jax.random.permutation(key, parts)[block_of(target)]
    other_side = (block_of(target) + parts // 2) % parts
    return jnp.where((block_of(source) == near) | (block_of(source) == other_side), factor * result, result)


def block_levels(key, dims, pieces, least, top_value):
    loudness = 1.0
    for axis_at, parts in pieces:
        heights = jax.random.uniform(jax.random.fold_in(jax.random.fold_in(key, 6), axis_at), (parts,), jnp.float32, least / len(pieces), top_value / len(pieces))
        loudness = loudness * jnp.repeat(jnp.exp(heights), dims[axis_at] // parts).reshape((-1,) + (1,) * (len(dims) - 1 - axis_at))
    return loudness


def normal_values(rng, extent, scale, limit, cuts=(), held_as=jnp.bfloat16):
    drawn = jax.random.normal(rng, extent, jnp.float32) * scale
    if len(cuts) > 0:
        drawn = block_levels(rng, extent, cuts, -0.22, 0.18) * drawn
    return jnp.clip(drawn, min=-limit, max=limit).astype(held_as)


def heavy_noise(key, extent, width, bound, cuts, heavy, kind=jnp.bfloat16):
    array = width * jax.random.normal(key, extent, jnp.float32)
    if cuts:
        array = array * block_levels(key, extent, cuts, -0.22, 0.18)
    return jnp.clip(strengthened(array, jax.random.fold_in(key, 3), *heavy), -bound, bound).astype(kind)


def setup_inputs(seed: int = 0) -> dict:
    streams_of = jax.random.split(jax.random.key(seed), 9)
    token_ids = plant(jax.random.randint(streams_of[0], (MICRO, SEQ), 0, VOCAB), jax.random.fold_in(streams_of[0], 1), 0, VOCAB - 1).astype(jnp.int32)
    emb_table = normal_values(streams_of[1], (VOCAB, D), 1.0, 6.0, ((0, 16), (1, 16)))
    attn_gain = jnp.clip(1.0 + 0.15 * jax.random.normal(streams_of[2], (LAYERS, D), jnp.float32), 0.25, 1.75).astype(jnp.bfloat16)
    query_weight = draw_query_weight(jax.random.fold_in(streams_of[8], 71), 0)
    key_weight = draw_key_weight(jax.random.fold_in(streams_of[8], 71), 0)
    value_weight = normal_values(streams_of[5], (LAYERS, D, HEADS * HEAD_DIM), D ** -0.5, 0.09375, ((0, 16), (2, 16)))
    mix_weight = jnp.clip(0.2 + 0.6 * jax.random.uniform(streams_of[6], (LAYERS, HEADS), jnp.float32) ** block_levels(streams_of[6], (LAYERS, HEADS), ((0, 16), (1, 16)), -0.2, 0.2), 0.2, 0.8)
    out_weight = heavy_noise(streams_of[7], (LAYERS, HEADS * HEAD_DIM, D), (HEADS * HEAD_DIM) ** -0.5, 0.125, ((0, 16), (1, 16)), (1, 2, 16, 2.0))
    return {"token_ids": token_ids, "emb_table": emb_table, "attn_gain": attn_gain, "query_weight": query_weight, "key_weight": key_weight, "value_weight": value_weight, "mix_weight": mix_weight, "out_weight": out_weight}


EPSILON = 1e-05
ROTARY_BASE = 10000.0

def rms_scale(values, norm_gain):
    mean_square = lax.optimization_barrier(jnp.mean(values * values, axis=-1, keepdims=True))
    return values * lax.rsqrt(mean_square + EPSILON) * norm_gain

def rotate(values):
    length = values.shape[-3]
    head_dim = values.shape[-1]
    half_dim = head_dim // 2
    positions = jnp.arange(length, dtype=jnp.float32)
    frequency = ROTARY_BASE ** (-(jnp.arange(half_dim, dtype=jnp.float32) * 2.0) / head_dim)
    angles = positions[:, None] * frequency[None, :]
    cosine = jnp.cos(angles)[:, None, :]
    sine_table = jnp.sin(angles)[:, None, :]
    leading = values[..., :half_dim]
    second = values[..., half_dim:]
    return jnp.concatenate([leading * cosine - second * sine_table, second * cosine + leading * sine_table], axis=-1)

def attend(queries, key_rows, mixed_values):
    length = queries.shape[1]
    scores = jnp.einsum('mqhd,mkhd->mhqk', queries.astype(jnp.float32), key_rows.astype(jnp.float32)) * HEAD_DIM ** (-0.5)
    causal = jnp.arange(length)[:, None] >= jnp.arange(length)[None, :]
    scores = jnp.where(causal, scores, -1e+30)
    row_top = lax.optimization_barrier(jnp.max(scores, axis=-1, keepdims=True))
    expo = jnp.exp(scores - row_top)
    attn_probs = (expo / lax.optimization_barrier(jnp.sum(expo, axis=-1, keepdims=True))).astype(jnp.bfloat16)
    attended = jnp.einsum('mhqk,mkhd->mqhd', attn_probs.astype(jnp.float32), mixed_values.astype(jnp.float32))
    return attended.astype(jnp.bfloat16)

def reference(token_ids, emb_table, attn_gain, query_weight, key_weight, value_weight, mix_weight, out_weight):
    batches, length = token_ids.shape
    first_rows = jnp.take(emb_table, token_ids.reshape(-1).astype(jnp.int32), axis=0)
    first_float = first_rows.astype(jnp.float32)
    first_norm = rms_scale(first_float, attn_gain[0].astype(jnp.float32)).astype(jnp.bfloat16)
    first_values = jnp.dot(first_norm, value_weight[0], preferred_element_type=jnp.float32).astype(jnp.bfloat16)
    source_values = first_values.reshape(batches, length, HEADS, HEAD_DIM).astype(jnp.float32)
    hidden = first_rows.reshape(batches, length, D)
    collected = []
    for layer_index in range(LAYERS):
        norm_gain = attn_gain[layer_index].astype(jnp.float32)
        normed = rms_scale(hidden.astype(jnp.float32), norm_gain).astype(jnp.bfloat16).reshape(-1, D)
        queries = jnp.dot(normed, query_weight[layer_index], preferred_element_type=jnp.float32)
        key_rows = jnp.dot(normed, key_weight[layer_index], preferred_element_type=jnp.float32)
        values = jnp.dot(normed, value_weight[layer_index], preferred_element_type=jnp.float32)
        queries = rotate(queries.reshape(batches, length, HEADS, HEAD_DIM)).astype(jnp.bfloat16)
        key_rows = rotate(key_rows.reshape(batches, length, HEADS, HEAD_DIM)).astype(jnp.bfloat16)
        values = values.reshape(batches, length, HEADS, HEAD_DIM)
        mix_rate = mix_weight[layer_index][:, None]
        mixed_values = (mix_rate * values + (1.0 - mix_rate) * source_values).astype(jnp.bfloat16)
        attended = attend(queries, key_rows, mixed_values).reshape(batches, length, N_TENSOR, -1)
        out_groups = out_weight[layer_index].reshape(N_TENSOR, -1, D)
        partial_value = jnp.einsum('msgc,gcd->gmsd', attended.astype(jnp.float32), out_groups.astype(jnp.float32))
        partial_value = lax.optimization_barrier(partial_value.astype(jnp.bfloat16)).astype(jnp.float32)
        summed = lax.optimization_barrier(jnp.sum(partial_value, axis=0))
        hidden = (hidden.astype(jnp.float32) + summed).astype(jnp.bfloat16)
        collected.append(hidden)
    return jnp.stack(collected)
```

```python
import functools

import jax
import jax.numpy as jnp
import numpy as np
from jax import lax
from jax.experimental import pallas as pl
from jax.experimental.pallas import tpu as pltpu
from jax.sharding import PartitionSpec as P

EPSILON = 1e-05
ROTARY_BASE = 10000.0
CHUNK = 16
MESH = pl.DeviceIdType.MESH
FAR_FIRST = (4, 3, -3, 2, -2, 1, -1, 0)
NEAR_FIRST_GROUPS = ((0, 1, -1), (2, -2), (3, -3), (4,))


def rotary_tables(length, head_dim):
    half = head_dim // 2
    frequency = ROTARY_BASE ** (-(np.arange(half, dtype=np.float32) * 2.0) / head_dim)
    angles = np.arange(length, dtype=np.float32)[:, None] * frequency[None, :].astype(np.float32)
    cosine, sine = np.cos(angles), np.sin(angles)
    return (
        np.concatenate([cosine, cosine], axis=1).astype(np.float32),
        np.concatenate([-sine, sine], axis=1).astype(np.float32),
    )


def kernel(
    sections, peers, length, head_local, head_dim,
    looked, gain_in, mix, cosine, sine, wq_in, wk_in, wv_in, wo_in,
    out,
    blocks, parts, parts_out, emb, fresh, first_values, k_cache, v_cache, gain, wq, wk, wv, wo,
    w_sem, x_sem, p_sem, e_sem, v_sem, xs_sem, ps_sem, es_sem, vs_sem,
):
    chunks, rows, width = looked.shape
    per_sequence = length // rows
    stacks = peers // 2
    s = lax.axis_index("section")
    t = lax.axis_index("tensor")
    z, core = t // 2, lax.rem(t, 2)

    def peer(dz, dc):
        return lax.rem(z + dz + stacks, stacks) * 2 + lax.rem(core + dc, 2)

    def weights():
        pairs = [(wq_in, wq, 0), (wk_in, wk, 1), (wv_in, wv, 2)]
        copies = [pltpu.make_async_copy(a, b, w_sem.at[i]) for a, b, i in pairs]
        for j in range(peers):
            copies.append(
                pltpu.make_async_copy(wo_in.at[0, :, pl.ds(j * width, width)], wo.at[j], w_sem.at[3 + j])
            )
        return copies

    def remote(src, dst, send, recv, section, tensor):
        return pltpu.make_async_remote_copy(
            src_ref=src, dst_ref=dst, send_sem=send, recv_sem=recv,
            device_id=(section, tensor), device_id_type=MESH,
        )

    def await_bytes(ref, sem):
        pltpu.make_async_copy(ref, ref, sem).wait()

    for copy in weights():
        copy.start()

    @pl.when(s != 0)
    def _():
        @pl.loop(0, chunks)
        def _(m):
            remote(looked.at[m], emb.at[m, s], es_sem.at[m], e_sem.at[m], 0, t).start()

    for j in range(peers):
        gain[j] = gain_in[:, j * width : (j + 1) * width].astype(jnp.float32)
    k_cache[...] = jnp.zeros_like(k_cache)
    v_cache[...] = jnp.zeros_like(v_cache)

    def embed(m):
        await_bytes(emb.at[m, pl.ds(1, sections - 1)], e_sem.at[m])
        total = looked[m].astype(jnp.float32)
        for j in range(1, sections):
            total += emb[m, j].astype(jnp.float32)
        blocks[m, t] = total.astype(jnp.bfloat16)
        for dz in FAR_FIRST:
            for dc in (1, 0):
                if (dz, dc) != (0, 0):
                    remote(
                        blocks.at[m, t], blocks.at[m, t], xs_sem.at[m], x_sem.at[m, t], 0, peer(dz, dc)
                    ).start()

    def compute(m):
        q = jnp.zeros((rows, width), jnp.float32)
        k = jnp.zeros((rows, width), jnp.float32)
        v = jnp.zeros((rows, width), jnp.float32)
        squares = jnp.zeros((rows, width), jnp.float32)
        for group in NEAR_FIRST_GROUPS:
            members = [(dz, dc) for dz in group for dc in (0, 1)]
            for dz, dc in members:
                j = peer(dz, dc)
                if (dz, dc) == (0, 0):
                    @pl.when(s != 0)
                    def _():
                        await_bytes(blocks.at[m, t], x_sem.at[m, t])
                else:
                    await_bytes(blocks.at[m, j], x_sem.at[m, j])
            for dz, dc in members:
                j = peer(dz, dc)
                x = blocks[m, j].astype(jnp.float32)
                squares += x * x
                scaled = (x * gain[j]).astype(jnp.bfloat16)
                q += jnp.dot(scaled, wq[j], preferred_element_type=jnp.float32)
                k += jnp.dot(scaled, wk[j], preferred_element_type=jnp.float32)
                v += jnp.dot(scaled, wv[j], preferred_element_type=jnp.float32)
        mean = jnp.sum(squares, axis=-1, keepdims=True) / (peers * width)
        scale = lax.rsqrt(mean + EPSILON)
        q, k, v = q * scale, k * scale, v * scale

        @pl.when(s == 0)
        def _():
            first_values[m] = v.astype(jnp.bfloat16)

        @pl.when(s != 0)
        def _():
            await_bytes(first_values.at[m], v_sem.at[m])

        @pl.when(s != sections - 1)
        def _():
            remote(first_values.at[m], first_values.at[m], vs_sem.at[m], v_sem.at[m], s + 1, t).start()

        source = first_values[m].astype(jnp.float32)
        at = pl.multiple_of(lax.rem(m, per_sequence) * rows, rows)
        cos_rows = cosine[pl.ds(at, rows), :]
        sin_rows = sine[pl.ds(at, rows), :]
        query_at = at + lax.broadcasted_iota(jnp.int32, (rows, length), 0)
        causal = query_at >= lax.broadcasted_iota(jnp.int32, (rows, length), 1)
        heads = []
        for h in range(head_local):
            lanes = slice(h * head_dim, (h + 1) * head_dim)
            qh, kh = q[:, lanes], k[:, lanes]
            qh = (qh * cos_rows + pltpu.roll(qh, head_dim // 2, 1) * sin_rows).astype(jnp.bfloat16)
            kh = (kh * cos_rows + pltpu.roll(kh, head_dim // 2, 1) * sin_rows).astype(jnp.bfloat16)
            rate = mix[0, h]
            vh = (rate * v[:, lanes] + (1.0 - rate) * source[:, lanes]).astype(jnp.bfloat16)
            k_cache[h, pl.ds(at, rows), :] = kh
            v_cache[h, pl.ds(at, rows), :] = vh
            scores = lax.dot_general(
                qh, k_cache[h], (((1,), (1,)), ((), ())), preferred_element_type=jnp.float32
            ) * head_dim ** (-0.5)
            scores = jnp.where(causal, scores, -1e30)
            expo = jnp.exp(scores - jnp.max(scores, axis=-1, keepdims=True))
            probs = (expo / jnp.sum(expo, axis=-1, keepdims=True)).astype(jnp.bfloat16)
            heads.append(jnp.dot(probs, v_cache[h], preferred_element_type=jnp.float32))
        attended = jnp.concatenate(heads, axis=1).astype(jnp.bfloat16)
        for dz in FAR_FIRST:
            for dc in (1, 0):
                j = peer(dz, dc)
                part = jnp.dot(attended, wo[j], preferred_element_type=jnp.float32).astype(jnp.bfloat16)
                if (dz, dc) == (0, 0):
                    parts[m, t] = part
                else:
                    parts_out[m, j] = part
                    remote(
                        parts_out.at[m, j], parts.at[m, t], ps_sem.at[m], p_sem.at[m], s, j
                    ).start()

    def reduce(m):
        await_bytes(parts.at[m, pl.ds(1, peers - 1)], p_sem.at[m])
        total = parts[m, 0].astype(jnp.float32)
        for j in range(1, peers):
            total += parts[m, j].astype(jnp.float32)
        hidden = (blocks[m, t].astype(jnp.float32) + total).astype(jnp.bfloat16)
        out[m] = hidden

        @pl.when(s != sections - 1)
        def _():
            fresh[m] = hidden
            for dz in FAR_FIRST:
                for dc in (1, 0):
                    remote(
                        fresh.at[m], blocks.at[m, t], xs_sem.at[m], x_sem.at[m, t], s + 1, peer(dz, dc)
                    ).start()

    @pl.when(s == 0)
    def _():
        embed(0)

    for copy in weights():
        copy.wait()

    @pl.loop(0, chunks)
    def _(i):
        @pl.when((s == 0) & (i + 1 < chunks))
        def _():
            embed(i + 1)

        compute(i)

        @pl.when(i >= 1)
        def _():
            reduce(i - 1)

    reduce(chunks - 1)

    @pl.loop(0, chunks)
    def _(m):
        await_bytes(parts_out.at[m, pl.ds(1, peers - 1)], ps_sem.at[m])

        @pl.when(s != 0)
        def _():
            await_bytes(looked.at[m], es_sem.at[m])

        @pl.when(s == 0)
        def _():
            await_bytes(blocks.at[m, pl.ds(1, peers - 1)], xs_sem.at[m])

        @pl.when(s != sections - 1)
        def _():
            await_bytes(first_values.at[m], vs_sem.at[m])
            await_bytes(blocks.at[m], xs_sem.at[m])


def shards(
    token_ids, emb_table, attn_gain, query_weight, key_weight, value_weight, mix_weight, out_weight
):
    section_rank = lax.axis_index("section")
    sections, peers = lax.axis_size("section"), lax.axis_size("tensor")
    batches, length = token_ids.shape
    vocab_local, width = emb_table.shape
    head_local = mix_weight.shape[1]
    head_dim = query_weight.shape[2] // head_local
    chunks = batches * length // CHUNK
    flat_ids = token_ids.reshape(-1) - section_rank * vocab_local
    one_hot = (flat_ids[:, None] == jnp.arange(vocab_local, dtype=jnp.int32)[None, :]).astype(
        jnp.bfloat16
    )
    looked = jnp.dot(one_hot, emb_table, preferred_element_type=jnp.float32)
    looked = looked.astype(jnp.bfloat16).reshape(chunks, CHUNK, width)
    cosine, sine = rotary_tables(length, head_dim)
    tiles = (peers, width, width)
    vmem, anywhere = pl.BlockSpec(memory_space=pltpu.VMEM), pl.BlockSpec(memory_space=pl.ANY)
    bf16, dma = jnp.bfloat16, pltpu.SemaphoreType.DMA
    result = pl.pallas_call(
        functools.partial(kernel, sections, peers, length, head_local, head_dim),
        out_shape=jax.ShapeDtypeStruct((chunks, CHUNK, width), bf16),
        in_specs=[vmem, vmem, pl.BlockSpec(memory_space=pltpu.SMEM), vmem, vmem] + [anywhere] * 4,
        out_specs=vmem,
        scratch_shapes=[
            pltpu.VMEM((chunks, peers, CHUNK, width), bf16),
            pltpu.VMEM((chunks, peers, CHUNK, width), bf16),
            pltpu.VMEM((chunks, peers, CHUNK, width), bf16),
            pltpu.VMEM((chunks, sections, CHUNK, width), bf16),
            pltpu.VMEM((chunks, CHUNK, width), bf16),
            pltpu.VMEM((chunks, CHUNK, width), bf16),
            pltpu.VMEM((head_local, length, head_dim), bf16),
            pltpu.VMEM((head_local, length, head_dim), bf16),
            pltpu.VMEM((peers, 1, width), jnp.float32),
            pltpu.VMEM(tiles, bf16),
            pltpu.VMEM(tiles, bf16),
            pltpu.VMEM(tiles, bf16),
            pltpu.VMEM(tiles, bf16),
            dma((3 + peers,)),
            dma((chunks, peers)),
            dma((chunks,)),
            dma((chunks,)),
            dma((chunks,)),
            dma((chunks,)),
            dma((chunks,)),
            dma((chunks,)),
            dma((chunks,)),
        ],
        compiler_params=pltpu.CompilerParams(has_side_effects=True, vmem_limit_bytes=40 * 2**20),
        name="relay",
    )(
        looked, attn_gain, mix_weight, jnp.asarray(cosine), jnp.asarray(sine),
        query_weight.reshape(tiles), key_weight.reshape(tiles), value_weight.reshape(tiles), out_weight,
    )
    return result.reshape(1, batches, length, width)


def solution(mesh):
    in_specs = (
        P(),
        P("section", "tensor"),
        P("section", None),
        P("section", None, "tensor"),
        P("section", None, "tensor"),
        P("section", None, "tensor"),
        P("section", "tensor"),
        P("section", "tensor", None),
    )
    out_specs = P("section", None, None, "tensor")
    return jax.shard_map(shards, mesh=mesh, in_specs=in_specs, out_specs=out_specs, check_vma=False)
```
